128 devices in a mesh: mat: 4 (over x), row: 8 (over z, y_hi), col: 2 (over core), dep: 2 (over y_lo).
Axes of the slice: x: 4, y: 4 (y_hi: 2, y_lo: 2; y = y_hi * 2 + y_lo), z: 4, core: 2. Of those that a mesh axis runs over, the one named last changes fastest.
Arguments:
- iterate: bfloat16 [8192, 14336], P('mat', ('row', 'col', 'dep')), parts along dimension 0, may hold values from -0.03125 to 0.03125
Outputs:
- update: bfloat16 [8192, 14336], P('mat', ('row', 'col', 'dep')), parts along dimension 0
The draws below stay inside these ranges and needn't reach their ends.
There are 4 independent parts, one for each index of `mat`. The reference program is written for one: setup_inputs(seed, part) draws one part's arguments, and reference() takes and returns one part's arrays. A program takes and returns all parts, laid end to end along the dimension named above; each array names one. Nothing has to cross between parts.
All inputs are finite; a program needn't handle non-finite values.
Results may differ from the reference program's by a relative error of at most 0.0059.
Values may be sent and summed in bfloat16 or wider, within the bound.
A program may use at most 128 MiB of HBM per device.

```python
import math
import jax
import jax.numpy as jnp

FF = 14336
ROWS = 2048


def steps_of(rng, extent, cuts, low, largest):
    def one(axis_at, blocks):
        heights = jax.random.uniform(jax.random.fold_in(jax.random.fold_in(rng, 6), axis_at), (blocks,), jnp.float32, low / len(cuts), largest / len(cuts))
        return jnp.repeat(jnp.exp(heights), extent[axis_at] // blocks).reshape((-1,) + (1,) * (len(extent) - axis_at - 1))

    gain = one(*cuts[0])
    for cut in cuts[1:]:
        gain = gain * one(*cut)
    return gain


def gaussian(own_key, dims, scale, limit, cuts=(), kind=jnp.bfloat16):
    gain = steps_of(own_key, dims, cuts, -0.22, 0.18) if cuts else 1.0
    values = jax.random.normal(own_key, dims, jnp.float32) * scale * gain
    return jnp.minimum(jnp.maximum(values, -limit), limit).astype(kind)


def setup_inputs(seed: int = 0, part: int = 0) -> dict:
    splits = jax.random.split(jax.random.key(seed), 2)
    part_keys = jax.random.split(jax.random.fold_in(splits[1], part), 2)
    return {
        "iterate": gaussian(part_keys[0], (ROWS, FF), (2 * FF) ** -0.5, 0.03125, ((1, 32),)),
    }


coef_a = 3.4445
coef_b = -4.775
coef_c = 2.0315

def reference(iterate):
    gram = jnp.dot(iterate, iterate.T, preferred_element_type=jnp.float32).astype(jnp.bfloat16)
    square = jnp.dot(gram, gram, preferred_element_type=jnp.float32)
    poly = (coef_b * gram.astype(jnp.float32) + coef_c * square).astype(jnp.bfloat16)
    applied = jnp.dot(poly, iterate, preferred_element_type=jnp.float32)
    updated = coef_a * iterate.astype(jnp.float32) + applied
    return (math.sqrt(FF) * updated).astype(jnp.bfloat16)
```

```python
import functools
import math

import jax
import jax.numpy as jnp
from jax import lax
from jax.experimental import pallas as pl
from jax.experimental.pallas import tpu as pltpu
from jax.sharding import PartitionSpec as P

FF = 14336
MESH = pl.DeviceIdType.MESH
BF16 = jnp.bfloat16
F32 = jnp.float32

coef_a = 3.4445
coef_b = -4.775
coef_c = 2.0315

STRIP = 128
MAIN = 256
EXTRA = 16
PIECE = MAIN + EXTRA
HALF = 144
OFFS = (2, 1, 3, 0)
UP = (0, 2)
DOWN = (1, 3)


def nt(a, b):
    return lax.dot_general(a, b, (((1,), (1,)), ((), ())), preferred_element_type=F32)


def kernel(cols, x_hbm, o_hbm, xt, x2, cf, s1, rr1, rn1, r1, s2, rr2, rn2, gs, g, yf, yb, ob, ssem, rsem, lsem):
    m, r, c, d = (lax.axis_index(a) for a in ("mat", "row", "col", "dep"))
    z = r // 2
    y = lax.rem(r, 2) * 2 + d
    depth = xt.shape[0]

    def mod4(v):
        return lax.rem(v, 4)

    def dev(yy, zz, cc):
        return (m, zz * 2 + yy // 2, cc, lax.rem(yy, 2))

    y_up, y_down = dev(mod4(y + 1), z, c), dev(mod4(y + 3), z, c)
    z_up, z_down = dev(y, mod4(z + 1), c), dev(y, mod4(z + 3), c)
    mate = dev(y, z, 1 - c)
    pos = ((y, z), (z, y))
    links = (((y_up, y_down), (z_up, z_down)), ((z_up, z_down), (y_up, y_down)))

    count = [0]
    started = []

    def send(src, dst, to):
        k = count[0]
        count[0] += 1
        copy = pltpu.make_async_remote_copy(
            src_ref=src, dst_ref=dst, send_sem=ssem.at[k], recv_sem=rsem.at[k], device_id=to, device_id_type=MESH
        )
        copy.start()
        started.append(copy)
        return copy

    load = pltpu.make_async_copy(x_hbm, xt.at[pl.ds(0, cols)], lsem.at[0])
    load.start()
    barrier = pltpu.get_barrier_semaphore()
    for other in (y_up, y_down, z_up, z_down, mate):
        pl.semaphore_signal(barrier, inc=1, device_id=other, device_id_type=MESH)
    if depth > cols:
        xt[cols:, :] = jnp.zeros((depth - cols, xt.shape[1]), BF16)
    load.wait()
    pl.semaphore_wait(barrier, 5)

    n_rows = xt.shape[1]
    half_rows = n_rows // 2
    swaps = []
    for part in range(2):
        for s in range(8):
            row = part * half_rows + s * STRIP
            there = pl.multiple_of(lax.rem(row + half_rows * c, n_rows), STRIP)
            x2[row : row + STRIP, 0:depth] = xt[:, pl.ds(there, STRIP)].T
        swaps.append(
            send(
                x2.at[pl.ds(part * half_rows, half_rows), pl.ds(0, depth)],
                x2.at[pl.ds((1 - part) * half_rows, half_rows), pl.ds(depth, depth)],
                mate,
            )
        )
    for copy in swaps:
        copy.wait_recv()

    def gram(h, j):
        u = 4 * h + mod4(pos[h][0] + OFFS[j])
        top = pl.multiple_of(u * STRIP, STRIP)
        main = nt(x2[pl.ds(top, 8 * STRIP), :], x2[pl.ds(top, STRIP), :])
        for t in range(4):
            cf[h, j, t, 0:MAIN] = main[t * MAIN : (t + 1) * MAIN]
        left = pl.multiple_of(u * STRIP + half_rows * (1 - c) + 64 * c, 64)
        right = pl.multiple_of(u * STRIP + half_rows * c, STRIP)
        extra = nt(x2[pl.ds(left, 64), :], x2[pl.ds(right, STRIP), :])
        for t in range(4):
            cf[h, j, t, MAIN:PIECE] = extra[t * EXTRA : (t + 1) * EXTRA]

    def mine(h, j, k):
        return cf[h, j, mod4(pos[h][1] + OFFS[k])]

    relay = {}
    near = {}
    for h in range(2):
        up, down = links[h][0]
        gram(h, 0)
        for i in range(2):
            for k, to, w in ((UP[i], up, 0), (DOWN[i], down, 1)):
                s1[h, 0, k] = mine(h, 0, k).astype(BF16)
                relay[h, w, k] = send(s1.at[h, 0, k], rr1.at[h, w, i], to)
    for h in range(2):
        up, down = links[h][0]
        for j, to, w, plain in ((1, up, 0, DOWN), (2, down, 1, UP)):
            gram(h, j)
            for k in plain:
                s1[h, j, k] = mine(h, j, k).astype(BF16)
                near[h, w, k] = send(s1.at[h, j, k], rn1.at[h, w, k], to)
    for i in range(2):
        for h in range(2):
            up, down = links[h][0]
            for j, to, w, k in ((1, up, 0, UP[i]), (2, down, 1, DOWN[i])):
                relay[h, w, k].wait_recv()
                s1[h, j, k] = (mine(h, j, k) + rr1[h, w, i].astype(F32)).astype(BF16)
                near[h, w, k] = send(s1.at[h, j, k], rn1.at[h, w, k], to)
    for h in range(2):
        gram(h, 3)

    relay2 = {}
    near2 = {}
    a_rows, b_rows = pl.ds(0, HALF), pl.ds(HALF, PIECE - HALF)
    for k in range(3):
        for h in range(2):
            up, down = links[h][1]
            near[h, 0, k].wait_recv()
            near[h, 1, k].wait_recv()
            total = mine(h, 3, k) + rn1[h, 0, k].astype(F32) + rn1[h, 1, k].astype(F32)
            if k == 0:
                s2[h, 0] = total.astype(BF16)
                relay2[h, 0] = send(s2.at[h, 0, a_rows], rr2.at[h, 0, a_rows], up)
                relay2[h, 1] = send(s2.at[h, 0, b_rows], rr2.at[h, 1, b_rows], down)
            elif k == 1:
                r1[h, 0] = total[:HALF]
                s2[h, 1, HALF:] = total[HALF:].astype(BF16)
                near2[h, 0, 1] = send(s2.at[h, 1, b_rows], rn2.at[h, 0, b_rows], up)
            else:
                r1[h, 1, : PIECE - HALF] = total[HALF:]
                s2[h, 2, :HALF] = total[:HALF].astype(BF16)
                near2[h, 1, 0] = send(s2.at[h, 2, a_rows], rn2.at[h, 1, a_rows], down)
    for h in range(2):
        up, down = links[h][1]
        relay2[h, 0].wait_recv()
        s2[h, 1, :HALF] = (r1[h, 0] + rr2[h, 0, :HALF].astype(F32)).astype(BF16)
        near2[h, 0, 0] = send(s2.at[h, 1, a_rows], rn2.at[h, 0, a_rows], up)
        relay2[h, 1].wait_recv()
        s2[h, 2, HALF:] = (r1[h, 1, : PIECE - HALF] + rr2[h, 1, HALF:].astype(F32)).astype(BF16)
        near2[h, 1, 1] = send(s2.at[h, 2, b_rows], rn2.at[h, 1, b_rows], down)
    for h in range(2):
        near[h, 0, 3].wait_recv()
        near[h, 1, 3].wait_recv()
        r1[h, 2] = (mine(h, 3, 3) + rn1[h, 0, 3].astype(F32) + rn1[h, 1, 3].astype(F32))[:HALF]
        r1[h, 3, : PIECE - HALF] = (mine(h, 3, 3) + rn1[h, 0, 3].astype(F32) + rn1[h, 1, 3].astype(F32))[HALF:]

    def slot(h, dp, dq, rows=None):
        p, q = mod4(pos[h][0] + dp), mod4(pos[h][1] + dq)
        ref = gs.at[c, h, p, q]
        return ref if rows is None else ref.at[rows]

    def push(h, dp, dq, to, rows=None):
        return send(slot(h, dp, dq, rows), slot(h, dp, dq, rows), to)

    def place(cc, h, dp, dq):
        p, q = mod4(pos[h][0] + dp), mod4(pos[h][1] + dq)
        uu = 4 * h + p
        u = 8 * cc + uu
        col = pl.multiple_of(u * STRIP, STRIP)
        for i in range(2):
            v = lax.rem(u + 2 * q + i, 16)
            row = pl.multiple_of(v * STRIP, STRIP)
            block = gs[cc, h, p, q, i * STRIP : (i + 1) * STRIP]
            g[pl.ds(row, STRIP), pl.ds(col, STRIP)] = block
            g[pl.ds(col, STRIP), pl.ds(row, STRIP)] = block.T
        row = pl.multiple_of((uu + 8) * STRIP + 64 * cc + EXTRA * q, EXTRA)
        ecol = pl.multiple_of(uu * STRIP, STRIP)
        g[pl.ds(row, EXTRA), pl.ds(ecol, STRIP)] = gs[cc, h, p, q, MAIN:PIECE]

    first, second, half, hop, cross = {}, {}, {}, {}, {}
    for h in range(2):
        (up1, down1), (up2, down2) = links[h]
        for w in range(2):
            near2[h, w, 0].wait_recv()
            near2[h, w, 1].wait_recv()
        here = rn2[h, 0].astype(F32) + rn2[h, 1].astype(F32)
        p, q = pos[h]
        gs[c, h, p, q, :HALF] = (r1[h, 2] + here[:HALF]).astype(BF16)
        gs[c, h, p, q, HALF:] = (r1[h, 3, : PIECE - HALF] + here[HALF:]).astype(BF16)
        first[h, 0] = push(h, 0, 0, up2)
        first[h, 1] = push(h, 0, 0, down2)
        second[h, 0, 0] = push(h, 0, 0, up1)
        second[h, 1, 0] = push(h, 0, 0, down1)
        cross[h, 0, 0] = push(h, 0, 0, mate)
    for h in range(2):
        (up1, down1), (up2, down2) = links[h]
        for w, dq, to, rows in ((0, 3, up2, a_rows), (1, 1, down2, b_rows)):
            first[h, w].wait_recv()
            half[h, w] = push(h, 0, dq, to, rows)
            second[h, 0, dq] = push(h, 0, dq, up1)
            second[h, 1, dq] = push(h, 0, dq, down1)
            cross[h, 0, dq] = push(h, 0, dq, mate)

    def arrive(h, dq):
        (up1, down1), _ = links[h]
        for w, dp, to, ahead in ((0, 3, up1, (0, 1)), (1, 1, down1, (3, 2))):
            second[h, w, dq].wait_recv()
            if dq in ahead:
                hop[h, dq] = push(h, dp, dq, to)
            cross[h, dp, dq] = push(h, dp, dq, mate)

    for h in range(2):
        arrive(h, 0)
    for h in range(2):
        (up1, down1), _ = links[h]
        half[h, 0].wait_recv()
        half[h, 1].wait_recv()
        second[h, 0, 2] = push(h, 0, 2, up1)
        second[h, 1, 2] = push(h, 0, 2, down1)
        cross[h, 0, 2] = push(h, 0, 2, mate)
    for dq in (1, 3):
        for h in range(2):
            arrive(h, dq)
    for h in range(2):
        for dq in (0, 1, 3):
            place(c, h, 0, dq)
    for h in range(2):
        arrive(h, 2)
    for h in range(2):
        for dp, dq in ((0, 2), (3, 0), (1, 0), (3, 1), (1, 1), (3, 3), (1, 3), (3, 2), (1, 2)):
            place(c, h, dp, dq)
    for h in range(2):
        for dq in (0, 1, 3, 2):
            hop[h, dq].wait_recv()
            cross[h, 2, dq] = push(h, 2, dq, mate)
    for h in range(2):
        for dp, dq in ((0, 0), (0, 3), (0, 1), (0, 2), (3, 0), (1, 0), (3, 1), (1, 1), (3, 3), (1, 3), (3, 2), (1, 2)):
            cross[h, dp, dq].wait_recv()
            place(1 - c, h, dp, dq)
    for h in range(2):
        for dq in (0, 1, 3, 2):
            place(c, h, 2, dq)
    for h in range(2):
        for dq in (0, 1, 3, 2):
            cross[h, 2, dq].wait_recv()
            place(1 - c, h, 2, dq)
    for uu in range(8):
        a, b = slice(uu * STRIP, (uu + 1) * STRIP), slice((uu + 8) * STRIP, (uu + 9) * STRIP)
        g[a, b] = g[b, a].T

    wide = 256
    x_t = xt[0:cols, :]

    @pl.loop(0, n_rows // wide)
    def _(n):
        at = pl.ds(pl.multiple_of(n * wide, wide), wide)
        part = jnp.dot(xt[0:cols, :], g[:, at], preferred_element_type=F32)
        yf[:, at] = part
        yb[:, at] = part.astype(BF16)

    scale = math.sqrt(FF)

    @pl.loop(0, n_rows // wide)
    def _(n):
        at = pl.ds(pl.multiple_of(n * wide, wide), wide)
        part = jnp.dot(yb[...], g[:, at], preferred_element_type=F32)
        updated = coef_a * xt[0:cols, at].astype(F32) + (coef_b * yf[:, at] + coef_c * part)
        ob[:, at] = (scale * updated).astype(BF16)
        pltpu.make_async_copy(ob.at[:, at], o_hbm.at[:, at], lsem.at[1 + n]).start()

    @pl.loop(0, n_rows // wide)
    def _(n):
        at = pl.ds(pl.multiple_of(n * wide, wide), wide)
        pltpu.make_async_copy(ob.at[:, at], o_hbm.at[:, at], lsem.at[1 + n]).wait()

    for copy in started:
        copy.wait_send()


def body(iterate):
    x = iterate.T
    cols, rows = x.shape
    depth = -(-cols // 128) * 128
    copies = 2 + 2 * (12 + 8 + 4 + 12 + 16)
    out = pl.pallas_call(
        functools.partial(kernel, cols),
        out_shape=jax.ShapeDtypeStruct((cols, rows), BF16),
        in_specs=[pl.BlockSpec(memory_space=pl.ANY)],
        out_specs=pl.BlockSpec(memory_space=pl.ANY),
        scratch_shapes=[
            pltpu.VMEM((depth, rows), BF16),
            pltpu.VMEM((rows, 2 * depth), BF16),
            pltpu.VMEM((2, 4, 4, PIECE, STRIP), F32),
            pltpu.VMEM((2, 3, 4, PIECE, STRIP), BF16),
            pltpu.VMEM((2, 2, 2, PIECE, STRIP), BF16),
            pltpu.VMEM((2, 2, 4, PIECE, STRIP), BF16),
            pltpu.VMEM((2, 4, HALF, STRIP), F32),
            pltpu.VMEM((2, 3, PIECE, STRIP), BF16),
            pltpu.VMEM((2, 2, PIECE, STRIP), BF16),
            pltpu.VMEM((2, 2, PIECE, STRIP), BF16),
            pltpu.VMEM((2, 2, 4, 4, PIECE, STRIP), BF16),
            pltpu.VMEM((rows, rows), BF16),
            pltpu.VMEM((cols, rows), F32),
            pltpu.VMEM((cols, rows), BF16),
            pltpu.VMEM((cols, rows), BF16),
            pltpu.SemaphoreType.DMA((copies,)),
            pltpu.SemaphoreType.DMA((copies,)),
            pltpu.SemaphoreType.DMA((1 + rows // 256,)),
        ],
        compiler_params=pltpu.CompilerParams(
            collective_id=0, has_side_effects=True, vmem_limit_bytes=60 * 1024 * 1024
        ),
    )(x)
    return out.T


def solution(mesh):
    spec = P("mat", ("row", "col", "dep"))
    return jax.shard_map(body, mesh=mesh, in_specs=(spec,), out_specs=spec, check_vma=False)
```

```python
import functools
import math

import jax
import jax.numpy as jnp
from jax import lax
from jax.experimental import pallas as pl
from jax.experimental.pallas import tpu as pltpu
from jax.sharding import PartitionSpec as P

FF = 14336
MESH = pl.DeviceIdType.MESH
BF16 = jnp.bfloat16
F32 = jnp.float32

coef_a = 3.4445
coef_b = -4.775
coef_c = 2.0315

STRIP = 128
EXTRA = 16
ROWS_OF = (STRIP, STRIP + EXTRA)
OFFS = (2, 3, 1, 0)
PAIR = 2 * STRIP


def nt(a, b):
    return lax.dot_general(a, b, (((1,), (1,)), ((), ())), preferred_element_type=F32)


def kernel(cols, x_hbm, o_hbm, xt, x2, cf0, cf1, s10, s11, rr10, rr11, rn10, rn11, r10, r11, s20, s21, rn20, rn21,
           gs0, gs1, g, yf, yb, ob, ssem, rsem, lsem):
    cf, s1, rr1, rn1, r1 = (cf0, cf1), (s10, s11), (rr10, rr11), (rn10, rn11), (r10, r11)
    s2, rn2, gs = (s20, s21), (rn20, rn21), (gs0, gs1)
    m, r, c, d = (lax.axis_index(a) for a in ("mat", "row", "col", "dep"))
    z = r // 2
    y = lax.rem(r, 2) * 2 + d
    depth, n_rows = xt.shape
    half_rows = n_rows // 2

    def mod4(v):
        return lax.rem(v, 4)

    def dev(yy, zz, cc):
        return (m, zz * 2 + yy // 2, cc, lax.rem(yy, 2))

    y_up, y_down = dev(mod4(y + 1), z, c), dev(mod4(y + 3), z, c)
    z_up, z_down = dev(y, mod4(z + 1), c), dev(y, mod4(z + 3), c)
    y_far, z_far = dev(mod4(y + 2), z, c), dev(y, mod4(z + 2), c)
    mate = dev(y, z, 1 - c)
    pos = ((y, z), (z, y))
    links = (((y_up, y_down), (z_up, z_down)), ((z_up, z_down), (y_up, y_down)))
    fars = ((y_far, z_far), (z_far, y_far))

    count = [0]
    started = []

    def send(src, dst, to):
        k = count[0]
        count[0] += 1
        copy = pltpu.make_async_remote_copy(
            src_ref=src, dst_ref=dst, send_sem=ssem.at[k], recv_sem=rsem.at[k], device_id=to, device_id_type=MESH
        )
        copy.start()
        started.append(copy)
        return copy

    loads = []
    for part in (1, 0):
        there = pl.ds(pl.multiple_of(lax.rem(part + c, 2) * half_rows, half_rows), half_rows)
        copy = pltpu.make_async_copy(x_hbm.at[:, there], xt.at[pl.ds(0, cols), there], lsem.at[part])
        copy.start()
        loads.append(copy)
    barrier = pltpu.get_barrier_semaphore()
    for other in (mate, y_up, y_down, z_up, z_down, y_far, z_far):
        pl.semaphore_signal(barrier, inc=1, device_id=other, device_id_type=MESH)
    if depth > cols:
        xt[cols:, :] = jnp.zeros((depth - cols, n_rows), BF16)
    swaps = {}
    for part, load in zip((1, 0), loads):
        load.wait()
        for s in range(half_rows // STRIP):
            row = part * half_rows + s * STRIP
            there = pl.multiple_of(lax.rem(row + half_rows * c, n_rows), STRIP)
            x2[row : row + STRIP, 0:depth] = xt[:, pl.ds(there, STRIP)].T
        if part == 1:
            pl.semaphore_wait(barrier, 7)
        swaps[part] = send(
            x2.at[pl.ds(part * half_rows, half_rows), pl.ds(0, depth)],
            x2.at[pl.ds((1 - part) * half_rows, half_rows), pl.ds(depth, depth)],
            mate,
        )

    def gram(e, h, which, part):
        pair = mod4(pos[h][0] + 2) // 2
        pair = pair if which == 0 else 1 - pair
        top = pl.multiple_of((4 * h + 2 * pair) * STRIP, PAIR)
        lanes = slice(part * depth, (part + 1) * depth)
        if e == 0:
            out = nt(x2[pl.ds(top, 5 * STRIP), lanes], x2[pl.ds(top, PAIR), lanes])
        else:
            out = nt(x2[pl.ds(top + 4 * STRIP, 6 * STRIP), lanes], x2[pl.ds(top, PAIR), lanes])
        for i in range(2):
            own = slice(i * STRIP, (i + 1) * STRIP)
            rows = [out[(i + q) * STRIP : (i + q + 1) * STRIP, own] for q in range(4)]
            if e == 1:
                block = out[(i + 4) * STRIP : (i + 5) * STRIP, own]
                extra = jnp.where(c == 0, block[:64], block.T[64:])
            for q in range(4):
                at = cf[e].at[h, 2 * pair + i, q]
                at[:STRIP] = rows[q] if part == 0 else at[:STRIP] + rows[q]
                if e == 1:
                    more = extra[q * EXTRA : (q + 1) * EXTRA]
                    at[STRIP:] = more if part == 0 else at[STRIP:] + more

    def mine(e, h, j, k):
        return cf[e][h, mod4(pos[h][0] + j), mod4(pos[h][1] + OFFS[k])]

    up_ks, down_ks = pl.ds(0, 2), pl.ds(2, 2)
    relay, near = {}, {}

    def relay_out(e, h):
        up, down = links[h][0]
        for k in range(4):
            s1[e][h, 0, k] = mine(e, h, 2, k).astype(BF16)
            if k == 1:
                relay[e, h, 0] = send(s1[e].at[h, 0, up_ks], rr1[e].at[h, 0], up)
        relay[e, h, 1] = send(s1[e].at[h, 0, down_ks], rr1[e].at[h, 1], down)

    def plain_out(e, h):
        up, down = links[h][0]
        for k in (2, 3):
            s1[e][h, 1, k] = mine(e, h, 1, k).astype(BF16)
        near[e, h, 0, 1] = send(s1[e].at[h, 1, down_ks], rn1[e].at[h, 0, down_ks], up)
        for k in (0, 1):
            s1[e][h, 2, k] = mine(e, h, 3, k).astype(BF16)
        near[e, h, 1, 0] = send(s1[e].at[h, 2, up_ks], rn1[e].at[h, 1, up_ks], down)

    def merged_out(e, h):
        up, down = links[h][0]
        relay[e, h, 0].wait_recv()
        for k in (0, 1):
            s1[e][h, 1, k] = (mine(e, h, 1, k) + rr1[e][h, 0, k].astype(F32)).astype(BF16)
        near[e, h, 0, 0] = send(s1[e].at[h, 1, up_ks], rn1[e].at[h, 0, up_ks], up)
        relay[e, h, 1].wait_recv()
        for k in (2, 3):
            s1[e][h, 2, k] = (mine(e, h, 3, k) + rr1[e][h, 1, k - 2].astype(F32)).astype(BF16)
        near[e, h, 1, 1] = send(s1[e].at[h, 2, down_ks], rn1[e].at[h, 1, down_ks], down)

    near2 = {}

    def ring2_first(e, h):
        up, down = links[h][1]

        def total(k):
            return mine(e, h, 0, k) + (rn1[e][h, 0, k].astype(F32) + rn1[e][h, 1, k].astype(F32))

        def out(k, w, to):
            s2[e][h, w] = total(k).astype(BF16)
            near2[e, h, w] = send(s2[e].at[h, w], rn2[e].at[h, w], to)

        near[e, h, 0, 1].wait_recv()
        near[e, h, 1, 0].wait_recv()
        near[e, h, 0, 0].wait_recv()
        out(0, 0, fars[h][1])
        out(1, 1, down)
        near[e, h, 1, 1].wait_recv()
        out(2, 2, up)
        r1[e][h] = total(3)

    first, second, hop, cross = {}, {}, {}, {}

    def push(e, h, dp, dq, to):
        ref = gs[e].at[c, h, mod4(pos[h][0] + dp), mod4(pos[h][1] + dq)]
        return send(ref, ref, to)

    def push_strip(e, h, dp):
        ref = gs[e].at[c, h, mod4(pos[h][0] + dp)]
        cross[e, h, dp] = send(ref, ref, mate)

    def push_near(e, h, dq):
        up, down = links[h][0]
        second[e, h, 0, dq] = push(e, h, 0, dq, up)
        second[e, h, 1, dq] = push(e, h, 0, dq, down)

    def ring2_own(e, h):
        up, down = links[h][1]
        for w in (1, 2, 0):
            near2[e, h, w].wait_recv()
        p, q = pos[h]
        others = rn2[e][h, 0].astype(F32) + (rn2[e][h, 1].astype(F32) + rn2[e][h, 2].astype(F32))
        gs[e][c, h, p, q] = (r1[e][h] + others).astype(BF16)
        first[e, h, 2] = push(e, h, 0, 0, fars[h][1])
        first[e, h, 3] = push(e, h, 0, 0, up)
        first[e, h, 1] = push(e, h, 0, 0, down)
        push_near(e, h, 0)

    def gather_sides(e, h):
        for dq in (3, 1):
            first[e, h, dq].wait_recv()
            push_near(e, h, dq)

    def gather_far(e, h):
        first[e, h, 2].wait_recv()
        hop[e, h, 2] = push(e, h, 0, 2, fars[h][0])
        push_near(e, h, 2)
        push_strip(e, h, 0)

    def arrive(e, h, dq):
        up, down = links[h][0]
        for w, dp, to, ahead in ((0, 3, up, (0, 1) if h == 0 else (1,)), (1, 1, down, (3,) if h == 0 else (0, 3))):
            second[e, h, w, dq].wait_recv()
            if dq in ahead:
                hop[e, h, dq] = push(e, h, dp, dq, to)
            if dq == 2:
                push_strip(e, h, dp)

    def hops(e, h):
        for dq in (0, 1, 3, 2):
            hop[e, h, dq].wait_recv()
        push_strip(e, h, 2)

    def place(e, cc, h, dp):
        p = mod4(pos[h][0] + dp)
        uu = 4 * h + p
        u = 8 * cc + uu
        col = pl.multiple_of(u * STRIP, STRIP)
        for q in range(4):
            row = pl.multiple_of(lax.rem(u + 4 * e + q, 16) * STRIP, STRIP)
            block = gs[e][cc, h, p, q, :STRIP]
            g[pl.ds(row, STRIP), pl.ds(col, STRIP)] = block
            g[pl.ds(col, STRIP), pl.ds(row, STRIP)] = block.T
            if e == 1:
                row = pl.multiple_of((uu + 8) * STRIP + 64 * cc + EXTRA * q, EXTRA)
                ecol = pl.multiple_of(uu * STRIP, STRIP)
                g[pl.ds(row, EXTRA), pl.ds(ecol, STRIP)] = gs[1][cc, h, p, q, STRIP:]

    def place_mate(e, h, dp):
        cross[e, h, dp].wait_recv()
        place(e, 1 - c, h, dp)

    def both(f, *args):
        for h in range(2):
            f(args[0], h, *args[1:])

    def times_g(left, n, pairs):
        runs = []
        for k in pairs:
            k %= n_rows // PAIR
            if runs and runs[-1][1] == k:
                runs[-1][1] = k + 1
            else:
                runs.append([k, k + 1])
        return sum(
            jnp.dot(left[0:cols, lo * PAIR : hi * PAIR], g[lo * PAIR : hi * PAIR, n * PAIR : (n + 1) * PAIR], preferred_element_type=F32)
            for lo, hi in runs
        )

    n_pairs = n_rows // PAIR
    for e in range(2):
        for which in range(2):
            for h in range(2):
                gram(e, h, which, 0)
    for h in range(2):
        swaps[1 - h].wait_recv()
        gram(0, h, 0, 1)
        relay_out(0, h)
    for h in range(2):
        gram(0, h, 1, 1)
        plain_out(0, h)
    for h in range(2):
        gram(1, h, 0, 1)
        relay_out(1, h)
    both(merged_out, 0)
    for h in range(2):
        gram(1, h, 1, 1)
        plain_out(1, h)
    both(merged_out, 1)
    both(ring2_first, 0)
    both(ring2_own, 0)
    both(ring2_first, 1)
    both(gather_sides, 0)
    both(arrive, 0, 0)
    both(gather_far, 0)
    both(ring2_own, 1)
    both(arrive, 0, 1)
    both(arrive, 0, 3)
    both(gather_sides, 1)
    both(arrive, 0, 2)
    both(arrive, 1, 0)
    both(gather_far, 1)
    for h in range(2):
        for dp in (0, 3, 1):
            place(0, c, h, dp)
    both(hops, 0)
    both(arrive, 1, 1)
    both(arrive, 1, 3)
    for dp in (0, 3, 1):
        both(place_mate, 0, dp)
    for h in range(2):
        place(0, c, h, 2)
    both(arrive, 1, 2)
    both(place_mate, 0, 2)
    for n in range(n_pairs):
        yf[:, n * PAIR : (n + 1) * PAIR] = times_g(xt, n, range(n - 1, n + 2))
    for h in range(2):
        for dp in (0, 3, 1):
            place(1, c, h, dp)
    both(hops, 1)
    for dp in (0, 3, 1):
        both(place_mate, 1, dp)
    for h in range(2):
        place(1, c, h, 2)
    both(place_mate, 1, 2)
    for uu in range(8):
        a, b = slice(uu * STRIP, (uu + 1) * STRIP), slice((uu + 8) * STRIP, (uu + 9) * STRIP)
        g[a, b] = g[b, a].T
    for n in range(n_pairs):
        at = slice(n * PAIR, (n + 1) * PAIR)
        part = yf[:, at] + times_g(xt, n, range(n + 2, n + n_pairs - 1))
        yf[:, at] = part
        yb[:, at] = part.astype(BF16)
    scale = math.sqrt(FF)
    outs = []
    for n in range(n_pairs):
        at = slice(n * PAIR, (n + 1) * PAIR)
        part = times_g(yb, n, range(n_pairs))
        updated = coef_a * xt[0:cols, at].astype(F32) + (coef_b * yf[:, at] + coef_c * part)
        ob[:, at] = (scale * updated).astype(BF16)
        lanes = pl.ds(n * PAIR, PAIR)
        copy = pltpu.make_async_copy(ob.at[:, lanes], o_hbm.at[:, lanes], lsem.at[2 + n])
        copy.start()
        outs.append(copy)
    for copy in outs:
        copy.wait()
    for copy in started:
        copy.wait_send()


def body(iterate):
    x = iterate.T
    cols, rows = x.shape
    depth = -(-cols // 128) * 128
    copies = 2 + 4 * (6 + 3 + 3 + 12 + 4)

    def each(*dims, dtype=BF16):
        return [pltpu.VMEM((*dims, n, STRIP), dtype) for n in ROWS_OF]

    out = pl.pallas_call(
        functools.partial(kernel, cols),
        out_shape=jax.ShapeDtypeStruct((cols, rows), BF16),
        in_specs=[pl.BlockSpec(memory_space=pl.ANY)],
        out_specs=pl.BlockSpec(memory_space=pl.ANY),
        scratch_shapes=[
            pltpu.VMEM((depth, rows), BF16),
            pltpu.VMEM((rows, 2 * depth), BF16),
            *each(2, 4, 4, dtype=F32),
            *each(2, 3, 4),
            *each(2, 2, 2),
            *each(2, 2, 4),
            *each(2, dtype=F32),
            *each(2, 3),
            *each(2, 3),
            *each(2, 2, 4, 4),
            pltpu.VMEM((rows, rows), BF16),
            pltpu.VMEM((cols, rows), F32),
            pltpu.VMEM((cols, rows), BF16),
            pltpu.VMEM((cols, rows), BF16),
            pltpu.SemaphoreType.DMA((copies,)),
            pltpu.SemaphoreType.DMA((copies,)),
            pltpu.SemaphoreType.DMA((2 + rows // PAIR,)),
        ],
        compiler_params=pltpu.CompilerParams(
            collective_id=0, has_side_effects=True, vmem_limit_bytes=60 * 1024 * 1024
        ),
    )(x)
    return out.T


def solution(mesh):
    spec = P("mat", ("row", "col", "dep"))
    return jax.shard_map(body, mesh=mesh, in_specs=(spec,), out_specs=spec, check_vma=False)
```

```python
import functools
import math

import jax
import jax.numpy as jnp
from jax import lax
from jax.experimental import pallas as pl
from jax.experimental.pallas import tpu as pltpu
from jax.sharding import PartitionSpec as P

FF = 14336
MESH = pl.DeviceIdType.MESH
BF16 = jnp.bfloat16
F32 = jnp.float32

coef_a = 3.4445
coef_b = -4.775
coef_c = 2.0315

STRIP = 128
EXTRA = 16
ROWS_OF = (STRIP, STRIP + EXTRA)
OFFS = (2, 3, 1, 0)
PAIR = 2 * STRIP


def nt(a, b):
    return lax.dot_general(a, b, (((1,), (1,)), ((), ())), preferred_element_type=F32)


def kernel(depth, x_hbm, o_ref, x_ref, x2, cf0, cf1, s10, s11, rr10, rr11, rn10, rn11, r10, r11, s20, s21, rn20, rn21,
           gs0, gs1, g, yf, yb, ssem, rsem, lsem):
    cf, s1, rr1, rn1, r1 = (cf0, cf1), (s10, s11), (rr10, rr11), (rn10, rn11), (r10, r11)
    s2, rn2, gs = (s20, s21), (rn20, rn21), (gs0, gs1)
    m, r, c, d = (lax.axis_index(a) for a in ("mat", "row", "col", "dep"))
    z = r // 2
    y = lax.rem(r, 2) * 2 + d
    cols, n_rows = x_ref.shape
    half_rows = n_rows // 2

    def mod4(v):
        return lax.rem(v, 4)

    def dev(yy, zz, cc):
        return (m, zz * 2 + yy // 2, cc, lax.rem(yy, 2))

    y_up, y_down = dev(mod4(y + 1), z, c), dev(mod4(y + 3), z, c)
    z_up, z_down = dev(y, mod4(z + 1), c), dev(y, mod4(z + 3), c)
    y_far, z_far = dev(mod4(y + 2), z, c), dev(y, mod4(z + 2), c)
    mate = dev(y, z, 1 - c)
    pos = ((y, z), (z, y))
    links = (((y_up, y_down), (z_up, z_down)), ((z_up, z_down), (y_up, y_down)))
    fars = ((y_far, z_far), (z_far, y_far))

    count = [0]
    started = []

    def send(src, dst, to):
        k = count[0]
        count[0] += 1
        copy = pltpu.make_async_remote_copy(
            src_ref=src, dst_ref=dst, send_sem=ssem.at[k], recv_sem=rsem.at[k], device_id=to, device_id_type=MESH
        )
        copy.start()
        started.append(copy)
        return copy

    loads = []
    for part in (1, 0):
        there = pl.ds(pl.multiple_of(lax.rem(part + c, 2) * half_rows, half_rows), half_rows)
        copy = pltpu.make_async_copy(x_hbm.at[:, there], x_ref.at[:, there], lsem.at[part])
        copy.start()
        loads.append(copy)
    barrier = pltpu.get_barrier_semaphore()
    for other in (mate, y_up, y_down, z_up, z_down, y_far, z_far):
        pl.semaphore_signal(barrier, inc=1, device_id=other, device_id_type=MESH)
    swaps = []
    for part, load in zip((1, 0), loads):
        load.wait()
        for s in range(half_rows // STRIP):
            row = part * half_rows + s * STRIP
            there = pl.multiple_of(lax.rem(row + half_rows * c, n_rows), STRIP)
            strip = x_ref[:, pl.ds(there, STRIP)]
            if depth > cols:
                strip = jnp.concatenate([strip, jnp.zeros((depth - cols, STRIP), BF16)], axis=0)
            x2[row : row + STRIP, 0:depth] = strip.T
        if part == 1:
            pl.semaphore_wait(barrier, 7)
        for at, n in ((half_rows, half_rows),) if part else ((0, half_rows // 2), (half_rows // 2, half_rows // 2)):
            swaps.append(
                send(
                    x2.at[pl.ds(at, n), pl.ds(0, depth)],
                    x2.at[pl.ds((at + half_rows) % n_rows, n), pl.ds(depth, depth)],
                    mate,
                )
            )

    def gram(e, h, which, part):
        pair = mod4(pos[h][0] + 2) // 2
        pair = pair if which == 0 else 1 - pair
        top = pl.multiple_of((4 * h + 2 * pair) * STRIP, PAIR)
        lanes = slice(part * depth, (part + 1) * depth)
        if e == 0:
            out = nt(x2[pl.ds(top, 5 * STRIP), lanes], x2[pl.ds(top, PAIR), lanes])
        else:
            out = nt(x2[pl.ds(top + 4 * STRIP, 6 * STRIP), lanes], x2[pl.ds(top, PAIR), lanes])
        for i in range(2):
            own = slice(i * STRIP, (i + 1) * STRIP)
            rows = [out[(i + q) * STRIP : (i + q + 1) * STRIP, own] for q in range(4)]
            if e == 1:
                block = out[(i + 4) * STRIP : (i + 5) * STRIP, own]
                extra = jnp.where(c == 0, block[:64], block.T[64:])
            for q in range(4):
                at = cf[e].at[h, 2 * pair + i, q]
                at[:STRIP] = rows[q] if part == 0 else at[:STRIP] + rows[q]
                if e == 1:
                    more = extra[q * EXTRA : (q + 1) * EXTRA]
                    at[STRIP:] = more if part == 0 else at[STRIP:] + more

    def mine(e, h, j, k):
        return cf[e][h, mod4(pos[h][0] + j), mod4(pos[h][1] + OFFS[k])]

    up_ks, down_ks = pl.ds(0, 2), pl.ds(2, 2)
    relay, near = {}, {}

    def relay_out(e, h):
        up, down = links[h][0]
        for k in range(4):
            s1[e][h, 0, k] = mine(e, h, 2, k).astype(BF16)
            if k == 1:
                relay[e, h, 0] = send(s1[e].at[h, 0, up_ks], rr1[e].at[h, 0], up)
        relay[e, h, 1] = send(s1[e].at[h, 0, down_ks], rr1[e].at[h, 1], down)

    def plain_out(e, h):
        up, down = links[h][0]
        for k in (2, 3):
            s1[e][h, 1, k] = mine(e, h, 1, k).astype(BF16)
        near[e, h, 0, 1] = send(s1[e].at[h, 1, down_ks], rn1[e].at[h, 0, down_ks], up)
        for k in (0, 1):
            s1[e][h, 2, k] = mine(e, h, 3, k).astype(BF16)
        near[e, h, 1, 0] = send(s1[e].at[h, 2, up_ks], rn1[e].at[h, 1, up_ks], down)

    def merged_out(e, h):
        up, down = links[h][0]
        relay[e, h, 0].wait_recv()
        for k in (0, 1):
            s1[e][h, 1, k] = (mine(e, h, 1, k) + rr1[e][h, 0, k].astype(F32)).astype(BF16)
        near[e, h, 0, 0] = send(s1[e].at[h, 1, up_ks], rn1[e].at[h, 0, up_ks], up)
        relay[e, h, 1].wait_recv()
        for k in (2, 3):
            s1[e][h, 2, k] = (mine(e, h, 3, k) + rr1[e][h, 1, k - 2].astype(F32)).astype(BF16)
        near[e, h, 1, 1] = send(s1[e].at[h, 2, down_ks], rn1[e].at[h, 1, down_ks], down)

    near2 = {}

    def ring2_first(e, h):
        up, down = links[h][1]

        def total(k):
            return mine(e, h, 0, k) + (rn1[e][h, 0, k].astype(F32) + rn1[e][h, 1, k].astype(F32))

        def out(k, w, to):
            s2[e][h, w] = total(k).astype(BF16)
            near2[e, h, w] = send(s2[e].at[h, w], rn2[e].at[h, w], to)

        near[e, h, 0, 1].wait_recv()
        near[e, h, 1, 0].wait_recv()
        near[e, h, 0, 0].wait_recv()
        out(0, 0, fars[h][1])
        out(1, 1, down)
        near[e, h, 1, 1].wait_recv()
        out(2, 2, up)
        r1[e][h] = total(3)

    first, second, hop, cross = {}, {}, {}, {}

    def push(e, h, dp, dq, to):
        ref = gs[e].at[c, h, mod4(pos[h][0] + dp), mod4(pos[h][1] + dq)]
        return send(ref, ref, to)

    def push_strip(e, h, dp):
        ref = gs[e].at[c, h, mod4(pos[h][0] + dp)]
        cross[e, h, dp] = send(ref, ref, mate)

    def push_near(e, h, dq):
        up, down = links[h][0]
        second[e, h, 0, dq] = push(e, h, 0, dq, up)
        second[e, h, 1, dq] = push(e, h, 0, dq, down)

    def ring2_own(e, h):
        up, down = links[h][1]
        for w in (1, 2, 0):
            near2[e, h, w].wait_recv()
        p, q = pos[h]
        others = rn2[e][h, 0].astype(F32) + (rn2[e][h, 1].astype(F32) + rn2[e][h, 2].astype(F32))
        gs[e][c, h, p, q] = (r1[e][h] + others).astype(BF16)
        first[e, h, 2] = push(e, h, 0, 0, fars[h][1])
        first[e, h, 3] = push(e, h, 0, 0, up)
        first[e, h, 1] = push(e, h, 0, 0, down)
        push_near(e, h, 0)

    def gather_sides(e, h):
        for dq in (3, 1):
            first[e, h, dq].wait_recv()
            push_near(e, h, dq)

    def gather_far(e, h):
        first[e, h, 2].wait_recv()
        hop[e, h, 2] = push(e, h, 0, 2, fars[h][0])
        push_near(e, h, 2)
        push_strip(e, h, 0)

    def arrive(e, h, dq):
        up, down = links[h][0]
        for w, dp, to, ahead in ((0, 3, up, (0, 1) if h == 0 else (1,)), (1, 1, down, (3,) if h == 0 else (0, 3))):
            second[e, h, w, dq].wait_recv()
            if dq in ahead:
                hop[e, h, dq] = push(e, h, dp, dq, to)
            if e == 1:
                cross[e, h, dp, dq] = push(e, h, dp, dq, mate)
            elif dq == 2:
                push_strip(e, h, dp)

    def hops(e, h):
        for dq in (0, 1, 3, 2):
            hop[e, h, dq].wait_recv()
            cross[e, h, 2, dq] = push(e, h, 2, dq, mate)

    def place(e, cc, h, dp):
        p = mod4(pos[h][0] + dp)
        uu = 4 * h + p
        u = 8 * cc + uu
        col = pl.multiple_of(u * STRIP, STRIP)
        for q in range(4):
            row = pl.multiple_of(lax.rem(u + 4 * e + q, 16) * STRIP, STRIP)
            block = gs[e][cc, h, p, q, :STRIP]
            g[pl.ds(row, STRIP), pl.ds(col, STRIP)] = block
            g[pl.ds(col, STRIP), pl.ds(row, STRIP)] = block.T
            if e == 1:
                row = pl.multiple_of((uu + 8) * STRIP + 64 * cc + EXTRA * q, EXTRA)
                ecol = pl.multiple_of(uu * STRIP, STRIP)
                g[pl.ds(row, EXTRA), pl.ds(ecol, STRIP)] = gs[1][cc, h, p, q, STRIP:]

    def place_mate(e, h, dp):
        for key in [k for k in cross if k[:3] == (e, h, dp)]:
            cross[key].wait_recv()
        place(e, 1 - c, h, dp)

    def both(f, *args):
        for h in range(2):
            f(args[0], h, *args[1:])

    def times_g(left, n, pairs):
        runs = []
        for k in pairs:
            k %= n_rows // PAIR
            if runs and runs[-1][1] == k:
                runs[-1][1] = k + 1
            else:
                runs.append([k, k + 1])
        return sum(
            jnp.dot(left[:, lo * PAIR : hi * PAIR], g[lo * PAIR : hi * PAIR, n * PAIR : (n + 1) * PAIR], preferred_element_type=F32)
            for lo, hi in runs
        )

    n_pairs = n_rows // PAIR
    for e in range(2):
        for which in range(2):
            for h in range(2):
                gram(e, h, which, 0)
    for h in range(2):
        swaps[h].wait_recv()
        gram(0, h, 0, 1)
        relay_out(0, h)
    for h in range(2):
        gram(0, h, 1, 1)
        plain_out(0, h)
    swaps[2].wait_recv()
    for h in range(2):
        gram(1, h, 0, 1)
        relay_out(1, h)
    both(merged_out, 0)
    for h in range(2):
        gram(1, h, 1, 1)
        plain_out(1, h)
    both(merged_out, 1)
    both(ring2_first, 0)
    both(ring2_first, 1)
    both(ring2_own, 0)
    both(ring2_own, 1)
    both(gather_sides, 0)
    both(arrive, 0, 0)
    both(gather_far, 0)
    both(gather_sides, 1)
    both(gather_far, 1)
    both(arrive, 0, 1)
    both(arrive, 0, 3)
    both(arrive, 1, 0)
    both(arrive, 0, 2)
    for h in range(2):
        for dp in (0, 3, 1):
            place(0, c, h, dp)
    both(place_mate, 0, 0)
    both(arrive, 1, 1)
    both(arrive, 1, 3)
    both(place_mate, 0, 3)
    both(place_mate, 0, 1)
    for h in range(2):
        place(1, c, h, 0)
    both(place_mate, 1, 0)
    both(hops, 0)
    for h in range(2):
        place(0, c, h, 2)
    both(arrive, 1, 2)
    for h in range(2):
        for dp in (3, 1):
            place(1, c, h, dp)
    both(place_mate, 0, 2)
    for n in range(n_pairs):
        yf[:, n * PAIR : (n + 1) * PAIR] = times_g(x_ref, n, range(n - 1, n + 2))
    both(hops, 1)
    for dp in (3, 1):
        both(place_mate, 1, dp)
    for h in range(2):
        place(1, c, h, 2)
    both(place_mate, 1, 2)
    for uu in range(8):
        a, b = slice(uu * STRIP, (uu + 1) * STRIP), slice((uu + 8) * STRIP, (uu + 9) * STRIP)
        g[a, b] = g[b, a].T
    scale = math.sqrt(FF)
    for n in range(n_pairs):
        at = slice(n * PAIR, (n + 1) * PAIR)
        part = yf[:, at] + times_g(x_ref, n, range(n + 2, n + n_pairs - 1))
        yb[:, at] = (scale * coef_c * part).astype(BF16)
        yf[:, at] = (scale * coef_a) * x_ref[:, at].astype(F32) + (scale * coef_b) * part
    for n in range(n_pairs):
        at = slice(n * PAIR, (n + 1) * PAIR)
        o_ref[:, at] = (yf[:, at] + times_g(yb, n, range(n_pairs))).astype(BF16)
    for copy in started:
        copy.wait_send()


def body(iterate):
    x = iterate.T
    cols, rows = x.shape
    depth = -(-cols // 128) * 128
    copies = 3 + 4 * (6 + 3 + 3 + 12 + 7) + 2 * 6

    def each(*dims, dtype=BF16):
        return [pltpu.VMEM((*dims, n, STRIP), dtype) for n in ROWS_OF]

    out = pl.pallas_call(
        functools.partial(kernel, depth),
        out_shape=jax.ShapeDtypeStruct((cols, rows), BF16),
        in_specs=[pl.BlockSpec(memory_space=pltpu.HBM)],
        out_specs=pl.BlockSpec(memory_space=pltpu.VMEM),
        scratch_shapes=[
            pltpu.VMEM((cols, rows), BF16),
            pltpu.VMEM((rows, 2 * depth), BF16),
            *each(2, 4, 4, dtype=F32),
            *each(2, 3, 4),
            *each(2, 2, 2),
            *each(2, 2, 4),
            *each(2, dtype=F32),
            *each(2, 3),
            *each(2, 3),
            *each(2, 2, 4, 4),
            pltpu.VMEM((rows, rows), BF16),
            pltpu.VMEM((cols, rows), F32),
            pltpu.VMEM((cols, rows), BF16),
            pltpu.SemaphoreType.DMA((copies,)),
            pltpu.SemaphoreType.DMA((copies,)),
            pltpu.SemaphoreType.DMA((2,)),
        ],
        compiler_params=pltpu.CompilerParams(
            collective_id=0, has_side_effects=True, vmem_limit_bytes=52 * 1024 * 1024
        ),
    )(x)
    return out.T


def solution(mesh):
    spec = P("mat", ("row", "col", "dep"))
    return jax.shard_map(body, mesh=mesh, in_specs=(spec,), out_specs=spec, check_vma=False)
```

```python
import functools
import math

import jax
import jax.numpy as jnp
from jax import lax
from jax.experimental import pallas as pl
from jax.experimental.pallas import tpu as pltpu
from jax.sharding import PartitionSpec as P

FF = 14336
MESH = pl.DeviceIdType.MESH
BF16 = jnp.bfloat16
F32 = jnp.float32

coef_a = 3.4445
coef_b = -4.775
coef_c = 2.0315

STRIP = 128
EXTRA = 16
ROWS_OF = (STRIP, STRIP + EXTRA)
OFFS = (2, 3, 1, 0)
PAIR = 2 * STRIP


def nt(a, b):
    return lax.dot_general(a, b, (((1,), (1,)), ((), ())), preferred_element_type=F32)


def kernel(depth, x_hbm, o_ref, x_ref, x2, cf0, cf1, s10, s11, rr10, rr11, rn10, rn11, r10, r11, s20, s21, rn20, rn21,
           gs0, gs1, g, yf, yb, ssem, rsem, lsem):
    cf, s1, rr1, rn1, r1 = (cf0, cf1), (s10, s11), (rr10, rr11), (rn10, rn11), (r10, r11)
    s2, rn2, gs = (s20, s21), (rn20, rn21), (gs0, gs1)
    m, r, c, d = (lax.axis_index(a) for a in ("mat", "row", "col", "dep"))
    z = r // 2
    y = lax.rem(r, 2) * 2 + d
    cols, n_rows = x_ref.shape
    half_rows = n_rows // 2

    def mod4(v):
        return lax.rem(v, 4)

    def dev(yy, zz, cc):
        return (m, zz * 2 + yy // 2, cc, lax.rem(yy, 2))

    y_up, y_down = dev(mod4(y + 1), z, c), dev(mod4(y + 3), z, c)
    z_up, z_down = dev(y, mod4(z + 1), c), dev(y, mod4(z + 3), c)
    y_far, z_far = dev(mod4(y + 2), z, c), dev(y, mod4(z + 2), c)
    mate = dev(y, z, 1 - c)
    pos = ((y, z), (z, y))
    links = (((y_up, y_down), (z_up, z_down)), ((z_up, z_down), (y_up, y_down)))
    fars = ((y_far, z_far), (z_far, y_far))
    sides = (dev(mod4(y + 1 + 2 * c), z, c), dev(y, mod4(z + 1 + 2 * c), c))

    count = [0]
    started = []

    def send(src, dst, to):
        k = count[0]
        count[0] += 1
        copy = pltpu.make_async_remote_copy(
            src_ref=src, dst_ref=dst, send_sem=ssem.at[k], recv_sem=rsem.at[k], device_id=to, device_id_type=MESH
        )
        copy.start()
        started.append(copy)
        return copy

    loads = []
    for part in (1, 0):
        there = pl.ds(pl.multiple_of(lax.rem(part + c, 2) * half_rows, half_rows), half_rows)
        copy = pltpu.make_async_copy(x_hbm.at[:, there], x_ref.at[:, there], lsem.at[part])
        copy.start()
        loads.append(copy)
    barrier = pltpu.get_barrier_semaphore()
    for other in (mate, y_up, y_down, z_up, z_down, y_far, z_far):
        pl.semaphore_signal(barrier, inc=1, device_id=other, device_id_type=MESH)
    swaps = []
    for part, load in zip((1, 0), loads):
        load.wait()
        for s in range(half_rows // STRIP):
            row = part * half_rows + s * STRIP
            there = pl.multiple_of(lax.rem(row + half_rows * c, n_rows), STRIP)
            strip = x_ref[:, pl.ds(there, STRIP)]
            if depth > cols:
                strip = jnp.concatenate([strip, jnp.zeros((depth - cols, STRIP), BF16)], axis=0)
            x2[row : row + STRIP, 0:depth] = strip.T
        if part == 1:
            pl.semaphore_wait(barrier, 7)
        for at, n in ((half_rows, half_rows),) if part else ((0, half_rows // 2), (half_rows // 2, half_rows // 2)):
            swaps.append(
                send(
                    x2.at[pl.ds(at, n), pl.ds(0, depth)],
                    x2.at[pl.ds((at + half_rows) % n_rows, n), pl.ds(depth, depth)],
                    mate,
                )
            )

    def gram(e, h, which, part):
        pair = mod4(pos[h][0] + 2) // 2
        pair = pair if which == 0 else 1 - pair
        top = pl.multiple_of((4 * h + 2 * pair) * STRIP, PAIR)
        lanes = slice(part * depth, (part + 1) * depth)
        if e == 0:
            out = nt(x2[pl.ds(top, 5 * STRIP), lanes], x2[pl.ds(top, PAIR), lanes])
        else:
            out = nt(x2[pl.ds(top + 4 * STRIP, 6 * STRIP), lanes], x2[pl.ds(top, PAIR), lanes])
        for i in range(2):
            own = slice(i * STRIP, (i + 1) * STRIP)
            rows = [out[(i + q) * STRIP : (i + q + 1) * STRIP, own] for q in range(4)]
            if e == 1:
                block = out[(i + 4) * STRIP : (i + 5) * STRIP, own]
                extra = jnp.where(c == 0, block[:64], block.T[64:])
            for q in range(4):
                at = cf[e].at[h, 2 * pair + i, q]
                at[:STRIP] = rows[q] if part == 0 else at[:STRIP] + rows[q]
                if e == 1:
                    more = extra[q * EXTRA : (q + 1) * EXTRA]
                    at[STRIP:] = more if part == 0 else at[STRIP:] + more

    def mine(e, h, j, k):
        return cf[e][h, mod4(pos[h][0] + j), mod4(pos[h][1] + OFFS[k])]

    up_ks, down_ks = pl.ds(0, 2), pl.ds(2, 2)
    relay, near = {}, {}

    def relay_out(e, h):
        up, down = links[h][0]
        for k in range(4):
            s1[e][h, 0, k] = mine(e, h, 2, k).astype(BF16)
            if k == 1:
                relay[e, h, 0] = send(s1[e].at[h, 0, up_ks], rr1[e].at[h, 0], up)
        relay[e, h, 1] = send(s1[e].at[h, 0, down_ks], rr1[e].at[h, 1], down)

    def plain_out(e, h):
        up, down = links[h][0]
        for k in (2, 3):
            s1[e][h, 1, k] = mine(e, h, 1, k).astype(BF16)
        near[e, h, 0, 1] = send(s1[e].at[h, 1, down_ks], rn1[e].at[h, 0, down_ks], up)
        for k in (0, 1):
            s1[e][h, 2, k] = mine(e, h, 3, k).astype(BF16)
        near[e, h, 1, 0] = send(s1[e].at[h, 2, up_ks], rn1[e].at[h, 1, up_ks], down)

    def merged_out(e, h):
        up, down = links[h][0]
        relay[e, h, 0].wait_recv()
        for k in (0, 1):
            s1[e][h, 1, k] = (mine(e, h, 1, k) + rr1[e][h, 0, k].astype(F32)).astype(BF16)
        near[e, h, 0, 0] = send(s1[e].at[h, 1, up_ks], rn1[e].at[h, 0, up_ks], up)
        relay[e, h, 1].wait_recv()
        for k in (2, 3):
            s1[e][h, 2, k] = (mine(e, h, 3, k) + rr1[e][h, 1, k - 2].astype(F32)).astype(BF16)
        near[e, h, 1, 1] = send(s1[e].at[h, 2, down_ks], rn1[e].at[h, 1, down_ks], down)

    near2 = {}

    def ring2_first(e, h):
        up, down = links[h][1]

        def total(k):
            return mine(e, h, 0, k) + (rn1[e][h, 0, k].astype(F32) + rn1[e][h, 1, k].astype(F32))

        def out(k, w, to):
            s2[e][h, w] = total(k).astype(BF16)
            near2[e, h, w] = send(s2[e].at[h, w], rn2[e].at[h, w], to)

        near[e, h, 0, 1].wait_recv()
        near[e, h, 1, 0].wait_recv()
        near[e, h, 0, 0].wait_recv()
        out(0, 0, fars[h][1])
        out(1, 1, down)
        near[e, h, 1, 1].wait_recv()
        out(2, 2, up)
        r1[e][h] = total(3)

    first, second, hop, cross = {}, {}, {}, {}

    def push(e, h, dp, dq, to):
        ref = gs[e].at[c, h, mod4(pos[h][0] + dp), mod4(pos[h][1] + dq)]
        return send(ref, ref, to)

    def push_strip(e, h, dp):
        ref = gs[e].at[c, h, mod4(pos[h][0] + dp)]
        cross[e, h, dp] = send(ref, ref, mate)

    def push_near(e, h, dq):
        up, down = links[h][0]
        second[e, h, 0, dq] = push(e, h, 0, dq, up)
        second[e, h, 1, dq] = push(e, h, 0, dq, down)

    def ring2_own(e, h):
        up, down = links[h][1]
        for w in (1, 2, 0):
            near2[e, h, w].wait_recv()
        p, q = pos[h]
        others = rn2[e][h, 0].astype(F32) + (rn2[e][h, 1].astype(F32) + rn2[e][h, 2].astype(F32))
        gs[e][c, h, p, q] = (r1[e][h] + others).astype(BF16)
        first[e, h, 2] = push(e, h, 0, 0, fars[h][1])
        first[e, h, 3] = push(e, h, 0, 0, up)
        first[e, h, 1] = push(e, h, 0, 0, down)
        push_near(e, h, 0)

    def gather_sides(e, h):
        for dq in (3, 1):
            first[e, h, dq].wait_recv()
            push_near(e, h, dq)

    def gather_far(e, h):
        first[e, h, 2].wait_recv()
        hop[e, h, 2] = push(e, h, 0, 2, fars[h][0])
        push_near(e, h, 2)
        push_strip(e, h, 0)

    def arrive(e, h, dq):
        up, down = links[h][0]
        for w, dp, to, ahead in ((0, 3, up, 1), (1, 1, down, 3)):
            second[e, h, w, dq].wait_recv()
            if dq == ahead:
                hop[e, h, dq] = push(e, h, dp, dq, to)
            if e == 1:
                cross[e, h, dp, dq] = push(e, h, dp, dq, mate)
            elif dq == 2:
                push_strip(e, h, dp)
        if dq == 0:
            hop[e, h, 0] = push(e, h, 3 - 2 * c, 0, sides[h])

    def hops(e, h):
        for dq in (0, 1, 3, 2):
            hop[e, h, dq].wait_recv()
            cross[e, h, 2, dq] = push(e, h, 2, dq, mate)

    def place(e, cc, h, dp):
        p = mod4(pos[h][0] + dp)
        uu = 4 * h + p
        u = 8 * cc + uu
        col = pl.multiple_of(u * STRIP, STRIP)
        for q in range(4):
            row = pl.multiple_of(lax.rem(u + 4 * e + q, 16) * STRIP, STRIP)
            block = gs[e][cc, h, p, q, :STRIP]
            g[pl.ds(row, STRIP), pl.ds(col, STRIP)] = block
            g[pl.ds(col, STRIP), pl.ds(row, STRIP)] = block.T
            if e == 1:
                row = pl.multiple_of((uu + 8) * STRIP + 64 * cc + EXTRA * q, EXTRA)
                ecol = pl.multiple_of(uu * STRIP, STRIP)
                g[pl.ds(row, EXTRA), pl.ds(ecol, STRIP)] = gs[1][cc, h, p, q, STRIP:]

    def place_mate(e, h, dp):
        for key in [k for k in cross if k[:3] == (e, h, dp)]:
            cross[key].wait_recv()
        place(e, 1 - c, h, dp)

    def both(f, *args):
        for h in range(2):
            f(args[0], h, *args[1:])

    def times_g(left, n, pairs):
        runs = []
        for k in pairs:
            k %= n_rows // PAIR
            if runs and runs[-1][1] == k:
                runs[-1][1] = k + 1
            else:
                runs.append([k, k + 1])
        return sum(
            jnp.dot(left[:, lo * PAIR : hi * PAIR], g[lo * PAIR : hi * PAIR, n * PAIR : (n + 1) * PAIR], preferred_element_type=F32)
            for lo, hi in runs
        )

    n_pairs = n_rows // PAIR
    for e in range(2):
        for which in range(2):
            for h in range(2):
                gram(e, h, which, 0)
    for h in range(2):
        swaps[h].wait_recv()
        gram(0, h, 0, 1)
        relay_out(0, h)
    for h in range(2):
        gram(0, h, 1, 1)
        plain_out(0, h)
    swaps[2].wait_recv()
    for h in range(2):
        gram(1, h, 0, 1)
        relay_out(1, h)
    both(merged_out, 0)
    for h in range(2):
        gram(1, h, 1, 1)
        plain_out(1, h)
    both(merged_out, 1)
    both(ring2_first, 0)
    both(ring2_first, 1)
    both(ring2_own, 0)
    both(ring2_own, 1)
    both(gather_sides, 0)
    both(arrive, 0, 0)
    both(gather_far, 0)
    both(gather_sides, 1)
    both(gather_far, 1)
    both(arrive, 0, 1)
    both(arrive, 0, 3)
    both(arrive, 1, 0)
    both(arrive, 0, 2)
    for h in range(2):
        for dp in (0, 3, 1):
            place(0, c, h, dp)
    both(place_mate, 0, 0)
    both(arrive, 1, 1)
    both(arrive, 1, 3)
    both(place_mate, 0, 3)
    both(place_mate, 0, 1)
    for h in range(2):
        place(1, c, h, 0)
    both(place_mate, 1, 0)
    both(hops, 0)
    for h in range(2):
        place(0, c, h, 2)
    both(arrive, 1, 2)
    for h in range(2):
        for dp in (3, 1):
            place(1, c, h, dp)
    both(place_mate, 0, 2)
    for n in range(n_pairs):
        yf[:, n * PAIR : (n + 1) * PAIR] = times_g(x_ref, n, range(n - 1, n + 2))
    both(hops, 1)
    for dp in (3, 1):
        both(place_mate, 1, dp)
    for h in range(2):
        place(1, c, h, 2)
    both(place_mate, 1, 2)
    for uu in range(8):
        a, b = slice(uu * STRIP, (uu + 1) * STRIP), slice((uu + 8) * STRIP, (uu + 9) * STRIP)
        g[a, b] = g[b, a].T
    scale = math.sqrt(FF)
    for n in range(n_pairs):
        at = slice(n * PAIR, (n + 1) * PAIR)
        part = yf[:, at] + times_g(x_ref, n, range(n + 2, n + n_pairs - 1))
        yb[:, at] = (scale * coef_c * part).astype(BF16)
        yf[:, at] = (scale * coef_a) * x_ref[:, at].astype(F32) + (scale * coef_b) * part
    for n in range(n_pairs):
        at = slice(n * PAIR, (n + 1) * PAIR)
        o_ref[:, at] = (yf[:, at] + times_g(yb, n, range(n_pairs))).astype(BF16)
    for copy in started:
        copy.wait_send()


def body(iterate):
    x = iterate.T
    cols, rows = x.shape
    depth = -(-cols // 128) * 128
    copies = 3 + 4 * (6 + 3 + 3 + 12 + 7) + 2 * 6

    def each(*dims, dtype=BF16):
        return [pltpu.VMEM((*dims, n, STRIP), dtype) for n in ROWS_OF]

    out = pl.pallas_call(
        functools.partial(kernel, depth),
        out_shape=jax.ShapeDtypeStruct((cols, rows), BF16),
        in_specs=[pl.BlockSpec(memory_space=pltpu.HBM)],
        out_specs=pl.BlockSpec(memory_space=pltpu.VMEM),
        scratch_shapes=[
            pltpu.VMEM((cols, rows), BF16),
            pltpu.VMEM((rows, 2 * depth), BF16),
            *each(2, 4, 4, dtype=F32),
            *each(2, 3, 4),
            *each(2, 2, 2),
            *each(2, 2, 4),
            *each(2, dtype=F32),
            *each(2, 3),
            *each(2, 3),
            *each(2, 2, 4, 4),
            pltpu.VMEM((rows, rows), BF16),
            pltpu.VMEM((cols, rows), F32),
            pltpu.VMEM((cols, rows), BF16),
            pltpu.SemaphoreType.DMA((copies,)),
            pltpu.SemaphoreType.DMA((copies,)),
            pltpu.SemaphoreType.DMA((2,)),
        ],
        compiler_params=pltpu.CompilerParams(
            collective_id=0, has_side_effects=True, vmem_limit_bytes=52 * 1024 * 1024
        ),
    )(x)
    return out.T


def solution(mesh):
    spec = P("mat", ("row", "col", "dep"))
    return jax.shard_map(body, mesh=mesh, in_specs=(spec,), out_specs=spec, check_vma=False)
```

```python
import functools
import math

import jax
import jax.numpy as jnp
from jax import lax
from jax.experimental import pallas as pl
from jax.experimental.pallas import tpu as pltpu
from jax.sharding import PartitionSpec as P

FF = 14336
MESH = pl.DeviceIdType.MESH
BF16 = jnp.bfloat16
F32 = jnp.float32

coef_a = 3.4445
coef_b = -4.775
coef_c = 2.0315

STRIP = 128
EXTRA = 16
ROWS_OF = (STRIP, STRIP + EXTRA)
OFFS = (2, 3, 1, 0)
PAIR = 2 * STRIP


def nt(a, b):
    return lax.dot_general(a, b, (((1,), (1,)), ((), ())), preferred_element_type=F32)


def kernel(depth, x_hbm, o_ref, x_ref, x2, cf0, cf1, s10, s11, rr10, rr11, rn10, rn11, r10, r11, s20, s21, rn20, rn21,
           gs0, gs1, g, yf, yb, ssem, rsem, lsem):
    cf, s1, rr1, rn1, r1 = (cf0, cf1), (s10, s11), (rr10, rr11), (rn10, rn11), (r10, r11)
    s2, rn2, gs = (s20, s21), (rn20, rn21), (gs0, gs1)
    m, r, c, d = (lax.axis_index(a) for a in ("mat", "row", "col", "dep"))
    z = r // 2
    y = lax.rem(r, 2) * 2 + d
    cols, n_rows = x_ref.shape
    half_rows = n_rows // 2

    def mod4(v):
        return lax.rem(v, 4)

    def dev(yy, zz, cc):
        return (m, zz * 2 + yy // 2, cc, lax.rem(yy, 2))

    y_up, y_down = dev(mod4(y + 1), z, c), dev(mod4(y + 3), z, c)
    z_up, z_down = dev(y, mod4(z + 1), c), dev(y, mod4(z + 3), c)
    y_far, z_far = dev(mod4(y + 2), z, c), dev(y, mod4(z + 2), c)
    mate = dev(y, z, 1 - c)
    pos = ((y, z), (z, y))
    links = (((y_up, y_down), (z_up, z_down)), ((z_up, z_down), (y_up, y_down)))
    fars = ((y_far, z_far), (z_far, y_far))
    sides = (dev(mod4(y + 1 + 2 * c), z, c), dev(y, mod4(z + 1 + 2 * c), c))
    backs = (dev(mod4(y + 3 - 2 * c), z, c), dev(y, mod4(z + 3 - 2 * c), c))

    count = [0]
    started = []

    def send(src, dst, to):
        k = count[0]
        count[0] += 1
        copy = pltpu.make_async_remote_copy(
            src_ref=src, dst_ref=dst, send_sem=ssem.at[k], recv_sem=rsem.at[k], device_id=to, device_id_type=MESH
        )
        copy.start()
        started.append(copy)
        return copy

    loads = []
    for part in (1, 0):
        there = pl.ds(pl.multiple_of(lax.rem(part + c, 2) * half_rows, half_rows), half_rows)
        copy = pltpu.make_async_copy(x_hbm.at[:, there], x_ref.at[:, there], lsem.at[part])
        copy.start()
        loads.append(copy)
    barrier = pltpu.get_barrier_semaphore()
    for other in (mate, y_up, y_down, z_up, z_down, y_far, z_far):
        pl.semaphore_signal(barrier, inc=1, device_id=other, device_id_type=MESH)
    swaps = []
    for part, load in zip((1, 0), loads):
        load.wait()
        for s in range(half_rows // STRIP):
            row = part * half_rows + s * STRIP
            there = pl.multiple_of(lax.rem(row + half_rows * c, n_rows), STRIP)
            strip = x_ref[:, pl.ds(there, STRIP)]
            if depth > cols:
                strip = jnp.concatenate([strip, jnp.zeros((depth - cols, STRIP), BF16)], axis=0)
            x2[row : row + STRIP, 0:depth] = strip.T
        if part == 1:
            pl.semaphore_wait(barrier, 7)
        for at, n in ((half_rows, half_rows),) if part else ((0, half_rows // 2), (half_rows // 2, half_rows // 2)):
            swaps.append(
                send(
                    x2.at[pl.ds(at, n), pl.ds(0, depth)],
                    x2.at[pl.ds((at + half_rows) % n_rows, n), pl.ds(depth, depth)],
                    mate,
                )
            )

    def gram(e, h, which, part):
        pair = mod4(pos[h][0] + 2) // 2
        pair = pair if which == 0 else 1 - pair
        top = pl.multiple_of((4 * h + 2 * pair) * STRIP, PAIR)
        lanes = slice(part * depth, (part + 1) * depth)
        if e == 0:
            out = nt(x2[pl.ds(top, 5 * STRIP), lanes], x2[pl.ds(top, PAIR), lanes])
        else:
            out = nt(x2[pl.ds(top + 4 * STRIP, 6 * STRIP), lanes], x2[pl.ds(top, PAIR), lanes])
        for i in range(2):
            own = slice(i * STRIP, (i + 1) * STRIP)
            rows = [out[(i + q) * STRIP : (i + q + 1) * STRIP, own] for q in range(4)]
            if e == 1:
                block = out[(i + 4) * STRIP : (i + 5) * STRIP, own]
                extra = jnp.where(c == 0, block[:64], block.T[64:])
            for q in range(4):
                at = cf[e].at[h, 2 * pair + i, q]
                at[:STRIP] = rows[q] if part == 0 else at[:STRIP] + rows[q]
                if e == 1:
                    more = extra[q * EXTRA : (q + 1) * EXTRA]
                    at[STRIP:] = more if part == 0 else at[STRIP:] + more

    def mine(e, h, j, k):
        return cf[e][h, mod4(pos[h][0] + j), mod4(pos[h][1] + OFFS[k])]

    up_ks, down_ks = pl.ds(0, 2), pl.ds(2, 2)
    relay, near = {}, {}

    def relay_out(e, h):
        up, down = links[h][0]
        for k in range(4):
            s1[e][h, 0, k] = mine(e, h, 2, k).astype(BF16)
            if k == 1:
                relay[e, h, 0] = send(s1[e].at[h, 0, up_ks], rr1[e].at[h, 0], up)
        relay[e, h, 1] = send(s1[e].at[h, 0, down_ks], rr1[e].at[h, 1], down)

    def plain_out(e, h):
        up, down = links[h][0]
        for k in (2, 3):
            s1[e][h, 1, k] = mine(e, h, 1, k).astype(BF16)
        near[e, h, 0, 1] = send(s1[e].at[h, 1, down_ks], rn1[e].at[h, 0, down_ks], up)
        for k in (0, 1):
            s1[e][h, 2, k] = mine(e, h, 3, k).astype(BF16)
        near[e, h, 1, 0] = send(s1[e].at[h, 2, up_ks], rn1[e].at[h, 1, up_ks], down)

    def merged_out(e, h):
        up, down = links[h][0]
        relay[e, h, 0].wait_recv()
        for k in (0, 1):
            s1[e][h, 1, k] = (mine(e, h, 1, k) + rr1[e][h, 0, k].astype(F32)).astype(BF16)
        near[e, h, 0, 0] = send(s1[e].at[h, 1, up_ks], rn1[e].at[h, 0, up_ks], up)
        relay[e, h, 1].wait_recv()
        for k in (2, 3):
            s1[e][h, 2, k] = (mine(e, h, 3, k) + rr1[e][h, 1, k - 2].astype(F32)).astype(BF16)
        near[e, h, 1, 1] = send(s1[e].at[h, 2, down_ks], rn1[e].at[h, 1, down_ks], down)

    near2 = {}

    def ring2_first(e, h):
        up, down = links[h][1]

        def total(k):
            return mine(e, h, 0, k) + (rn1[e][h, 0, k].astype(F32) + rn1[e][h, 1, k].astype(F32))

        def out(k, w, to):
            s2[e][h, w] = total(k).astype(BF16)
            near2[e, h, w] = send(s2[e].at[h, w], rn2[e].at[h, w], to)

        near[e, h, 0, 1].wait_recv()
        near[e, h, 1, 0].wait_recv()
        near[e, h, 0, 0].wait_recv()
        out(0, 0, fars[h][1])
        out(1, 1, down)
        near[e, h, 1, 1].wait_recv()
        out(2, 2, up)
        r1[e][h] = total(3)

    first, second, hop, cross = {}, {}, {}, {}

    def push(e, h, dp, dq, to):
        ref = gs[e].at[c, h, mod4(pos[h][0] + dp), mod4(pos[h][1] + dq)]
        return send(ref, ref, to)

    def push_strip(e, h, dp):
        ref = gs[e].at[c, h, mod4(pos[h][0] + dp)]
        cross[e, h, dp] = send(ref, ref, mate)

    def push_near(e, h, dq):
        up, down = links[h][0]
        second[e, h, 0, dq] = push(e, h, 0, dq, up)
        second[e, h, 1, dq] = push(e, h, 0, dq, down)

    def ring2_own(e, h):
        up, down = links[h][1]
        for w in (1, 2, 0):
            near2[e, h, w].wait_recv()
        p, q = pos[h]
        others = rn2[e][h, 0].astype(F32) + (rn2[e][h, 1].astype(F32) + rn2[e][h, 2].astype(F32))
        gs[e][c, h, p, q] = (r1[e][h] + others).astype(BF16)
        first[e, h, 2] = push(e, h, 0, 0, fars[h][1])
        first[e, h, 3] = push(e, h, 0, 0, up)
        first[e, h, 1] = push(e, h, 0, 0, down)
        push_near(e, h, 0)

    def gather_sides(e, h):
        for dq in (3, 1):
            first[e, h, dq].wait_recv()
            push_near(e, h, dq)

    def gather_far(e, h):
        first[e, h, 2].wait_recv()
        if e == 1:
            hop[e, h, 2] = push(e, h, 0, 2, fars[h][0])
        push_near(e, h, 2)
        push_strip(e, h, 0)

    def arrive(e, h, dq):
        up, down = links[h][0]
        for w, dp, to, ahead in ((0, 3, up, 1), (1, 1, down, 3)):
            second[e, h, w, dq].wait_recv()
            if dq == ahead:
                hop[e, h, dq] = push(e, h, dp, dq, to)
            if e == 1:
                cross[e, h, dp, dq] = push(e, h, dp, dq, mate)
            elif dq == 2:
                push_strip(e, h, dp)
        if dq == 0:
            hop[e, h, 0] = push(e, h, 3 - 2 * c, 0, sides[h])
        if dq == 2 and e == 0:
            hop[e, h, 2] = push(e, h, 1 + 2 * c, 2, backs[h])

    def hops(e, h):
        for dq in (0, 1, 3, 2):
            hop[e, h, dq].wait_recv()
            cross[e, h, 2, dq] = push(e, h, 2, dq, mate)

    def place(e, cc, h, dp):
        p = mod4(pos[h][0] + dp)
        uu = 4 * h + p
        u = 8 * cc + uu
        col = pl.multiple_of(u * STRIP, STRIP)
        for q in range(4):
            row = pl.multiple_of(lax.rem(u + 4 * e + q, 16) * STRIP, STRIP)
            block = gs[e][cc, h, p, q, :STRIP]
            g[pl.ds(row, STRIP), pl.ds(col, STRIP)] = block
            g[pl.ds(col, STRIP), pl.ds(row, STRIP)] = block.T
            if e == 1:
                row = pl.multiple_of((uu + 8) * STRIP + 64 * cc + EXTRA * q, EXTRA)
                ecol = pl.multiple_of(uu * STRIP, STRIP)
                g[pl.ds(row, EXTRA), pl.ds(ecol, STRIP)] = gs[1][cc, h, p, q, STRIP:]

    def place_mate(e, h, dp):
        for key in [k for k in cross if k[:3] == (e, h, dp)]:
            cross[key].wait_recv()
        place(e, 1 - c, h, dp)

    def both(f, *args):
        for h in range(2):
            f(args[0], h, *args[1:])

    def times_g(left, n, pairs):
        runs = []
        for k in pairs:
            k %= n_rows // PAIR
            if runs and runs[-1][1] == k:
                runs[-1][1] = k + 1
            else:
                runs.append([k, k + 1])
        return sum(
            jnp.dot(left[:, lo * PAIR : hi * PAIR], g[lo * PAIR : hi * PAIR, n * PAIR : (n + 1) * PAIR], preferred_element_type=F32)
            for lo, hi in runs
        )

    n_pairs = n_rows // PAIR
    for e in range(2):
        for which in range(2):
            for h in range(2):
                gram(e, h, which, 0)
    for h in range(2):
        swaps[h].wait_recv()
        gram(0, h, 0, 1)
        relay_out(0, h)
    for h in range(2):
        gram(0, h, 1, 1)
        plain_out(0, h)
    swaps[2].wait_recv()
    for h in range(2):
        gram(1, h, 0, 1)
        relay_out(1, h)
    both(merged_out, 0)
    for h in range(2):
        gram(1, h, 1, 1)
        plain_out(1, h)
    both(merged_out, 1)
    both(ring2_first, 0)
    both(ring2_first, 1)
    both(ring2_own, 0)
    both(ring2_own, 1)
    both(gather_sides, 0)
    both(arrive, 0, 0)
    both(gather_far, 0)
    both(gather_sides, 1)
    both(gather_far, 1)
    both(arrive, 0, 1)
    both(arrive, 0, 3)
    both(arrive, 1, 0)
    both(arrive, 0, 2)
    for h in range(2):
        for dp in (0, 3, 1):
            place(0, c, h, dp)
    both(place_mate, 0, 0)
    both(arrive, 1, 1)
    both(arrive, 1, 3)
    both(place_mate, 0, 3)
    both(place_mate, 0, 1)
    for h in range(2):
        place(1, c, h, 0)
    both(place_mate, 1, 0)
    both(hops, 0)
    for h in range(2):
        place(0, c, h, 2)
    both(arrive, 1, 2)
    for h in range(2):
        for dp in (3, 1):
            place(1, c, h, dp)
    both(place_mate, 0, 2)
    for n in range(n_pairs):
        yf[:, n * PAIR : (n + 1) * PAIR] = times_g(x_ref, n, range(n - 1, n + 2))
    both(hops, 1)
    for dp in (3, 1):
        both(place_mate, 1, dp)
    for h in range(2):
        place(1, c, h, 2)
    both(place_mate, 1, 2)
    for uu in range(8):
        a, b = slice(uu * STRIP, (uu + 1) * STRIP), slice((uu + 8) * STRIP, (uu + 9) * STRIP)
        g[a, b] = g[b, a].T
    scale = math.sqrt(FF)
    for n in range(n_pairs):
        at = slice(n * PAIR, (n + 1) * PAIR)
        part = yf[:, at] + times_g(x_ref, n, range(n + 2, n + n_pairs - 1))
        yb[:, at] = (scale * coef_c * part).astype(BF16)
        yf[:, at] = (scale * coef_a) * x_ref[:, at].astype(F32) + (scale * coef_b) * part
    for n in range(n_pairs):
        at = slice(n * PAIR, (n + 1) * PAIR)
        o_ref[:, at] = (yf[:, at] + times_g(yb, n, range(n_pairs))).astype(BF16)
    for copy in started:
        copy.wait_send()


def body(iterate):
    x = iterate.T
    cols, rows = x.shape
    depth = -(-cols // 128) * 128
    copies = 3 + 4 * (6 + 3 + 3 + 12 + 7) + 2 * 6

    def each(*dims, dtype=BF16):
        return [pltpu.VMEM((*dims, n, STRIP), dtype) for n in ROWS_OF]

    out = pl.pallas_call(
        functools.partial(kernel, depth),
        out_shape=jax.ShapeDtypeStruct((cols, rows), BF16),
        in_specs=[pl.BlockSpec(memory_space=pltpu.HBM)],
        out_specs=pl.BlockSpec(memory_space=pltpu.VMEM),
        scratch_shapes=[
            pltpu.VMEM((cols, rows), BF16),
            pltpu.VMEM((rows, 2 * depth), BF16),
            *each(2, 4, 4, dtype=F32),
            *each(2, 3, 4),
            *each(2, 2, 2),
            *each(2, 2, 4),
            *each(2, dtype=F32),
            *each(2, 3),
            *each(2, 3),
            *each(2, 2, 4, 4),
            pltpu.VMEM((rows, rows), BF16),
            pltpu.VMEM((cols, rows), F32),
            pltpu.VMEM((cols, rows), BF16),
            pltpu.SemaphoreType.DMA((copies,)),
            pltpu.SemaphoreType.DMA((copies,)),
            pltpu.SemaphoreType.DMA((2,)),
        ],
        compiler_params=pltpu.CompilerParams(
            collective_id=0, has_side_effects=True, vmem_limit_bytes=52 * 1024 * 1024
        ),
    )(x)
    return out.T


def solution(mesh):
    spec = P("mat", ("row", "col", "dep"))
    return jax.shard_map(body, mesh=mesh, in_specs=(spec,), out_specs=spec, check_vma=False)
```
